32 devices in a mesh: dp: 8 (over y, x, core), expert: 4 (over z).
Axes of the slice: x: 2, y: 2, z: 4, core: 2. Of those that a mesh axis runs over, the one named last changes fastest.
Arguments:
- policy_hidden: bfloat16 [1024, 4096], P('dp', 'expert'), may hold values from -6 to 6
- reference_hidden: bfloat16 [1024, 4096], P('dp', 'expert'), may hold values from -6 to 6
- policy_norm_gain: float32 [4096], P('expert'), may hold values from 0.25 to 1.75
- reference_norm_gain: float32 [4096], P('expert'), may hold values from 0.25 to 1.75
- policy_router: float32 [4096, 4], P('expert'), may hold values from -5.1875 to 5.1875
- reference_router: float32 [4096, 4], P('expert'), may hold values from -5.1875 to 5.1875
- policy_gate: bfloat16 [4, 4096, 8192], P('expert', 'dp'), may hold values from -0.09375 to 0.09375
- policy_up: bfloat16 [4, 4096, 8192], P('expert', 'dp'), may hold values from -0.09375 to 0.09375
- policy_down: bfloat16 [4, 8192, 4096], P('expert', 'dp'), may hold values from -0.0625 to 0.0625
- reference_gate: bfloat16 [4, 4096, 8192], P('expert', 'dp'), may hold values from -0.09375 to 0.09375
- reference_up: bfloat16 [4, 4096, 8192], P('expert', 'dp'), may hold values from -0.09375 to 0.09375
- reference_down: bfloat16 [4, 8192, 4096], P('expert', 'dp'), may hold values from -0.0625 to 0.0625
- expert_ids: int32 [1024, 2], P('dp'), may hold values from 0 to 3, all different within a row; in each aligned block of 128 rows (0 to 127, 128 to 255, ...) at most 96 rows name the same one
- lengths: int32 [32], P('dp'), may hold values from 1 to 32, as said below
Outputs:
- policy_mixture: bfloat16 [1024, 4096], P('dp', 'expert')
- reference_mixture: bfloat16 [1024, 4096], P('dp', 'expert')
- token_kl: float32 [1024], P('dp')
- loss: float32 [], replicated
The draws below stay inside these ranges and needn't reach their ends.
Inputs may be any that keep to these rules, and one draw needn't show every extreme that they name: `expert_ids`: each row names 2 different experts; among the rows of one index of dp (aligned blocks of 128 rows) no expert is named more than 96 times, and in some block one expert is named exactly 96 times. The first lengths[r] of rollout r's 32 positions are live.
All inputs are finite; a program needn't handle non-finite values.
Results may differ from the reference program's by a relative error of at most 0.02.
Values may be sent and summed in bfloat16 or wider, within the bound.
A program may use at most 256 MiB of HBM per device.

```python
import math
import jax
import jax.numpy as jnp
import numpy as np
from jax import lax

D = 4096
FF = 8192
TOP = 2
SEG = 32
TOK_DEV = 128
EXPERTS = 4
CAP = 96
TOKENS = 1024
N_DP = 8


def router_draw(key, stream_index):
    individual = jnp.clip(jax.random.normal(jax.random.fold_in(key, stream_index), (D, EXPERTS), jnp.float32), -4.0, 4.0) / math.sqrt(D)
    return individual


def draw_policy_router(key, part):
    return router_draw(key, 11)


def draw_reference_router(key, part):
    return router_draw(key, 12)


def draw_lengths(key, part):
    rollout_count = TOKENS // SEG
    per_block = TOK_DEV // SEG
    rollout_index = jnp.arange(rollout_count, dtype=jnp.int32)
    block_index = rollout_index // per_block
    block_total = rollout_count // per_block
    floor_limit = max(SEG // 3, 1)
    upper_limit = floor_limit + (SEG - floor_limit) * block_index // max(block_total - 1, 1)
    drawn = jax.random.randint(jax.random.fold_in(key, 5), (rollout_count,), 1, upper_limit + 1, dtype=jnp.int32)
    fullest = rollout_count - per_block
    drawn = jnp.where(rollout_index == fullest, jnp.int32(SEG), drawn)
    drawn = jnp.where(rollout_index == 0, jnp.int32(1), drawn)
    return drawn.astype(jnp.int32)


def levels(own_key, extent, pieces, low, high):
    level, own = 1.0, jax.random.fold_in(own_key, 6)
    for dim, parts in pieces:
        steps = jnp.exp(jax.random.uniform(jax.random.fold_in(own, dim), (parts,), jnp.float32, low / len(pieces), high / len(pieces)))
        level = level * jnp.repeat(steps, extent[dim] // parts).reshape([-1 if axis == dim else 1 for axis in range(len(extent))])
    return level


def deal_out(stream_key, own, number, rows, count, top, reach, lean):
    sequence = jax.random.permutation(stream_key, count)
    crowded, usual = load_shares(count, rows * top, reach, lean, True), load_shares(count, rows * top, reach, lean, False)
    places = jnp.arange(count)

    def named(sizes, turn):
        used = int((sizes > 0).sum())
        fixed = max(1, used // 4)
        passed = fixed + (places - fixed + turn * (used - fixed)) % max(1, count - fixed)
        return jnp.zeros((count,), jnp.int32).at[sequence[jnp.where(places < fixed, places, passed)]].set(jnp.asarray(sizes, jnp.int32))

    sizes = jnp.where(number % 4 == 0, named(crowded, number // 4), named(usual, number - number // 4 - 1))
    mixed = jax.random.permutation(jax.random.fold_in(own, 3), count)
    donor, sink = mixed[0:count // 2 * 2:2], mixed[1:count // 2 * 2:2]
    margin = jnp.minimum(sizes[donor] - 1, reach - sizes[sink]) // 2
    margin = jnp.where((donor == sequence[0]) | (sink == sequence[0]) | (sizes[sink] == 0), 0, jnp.maximum(margin, 0))
    passed = jax.random.randint(jax.random.fold_in(own, 4), (count // 2,), 0, 1 << 20) % (margin + 1)
    sizes = sizes.at[donor].add(-passed).at[sink].add(passed)
    labels = jnp.searchsorted(jnp.cumsum(sizes), jnp.arange(rows * top), side="right").astype(jnp.int32)
    listing = labels.reshape(top, rows).T
    listing = listing[jax.random.permutation(jax.random.fold_in(own, 1), rows)]
    turn = jax.random.randint(jax.random.fold_in(own, 2), (rows, 1), 0, top)
    return jnp.take_along_axis(listing, (jnp.arange(top)[None, :] + turn) % top, axis=1)


def load_shares(count, total, reach, lean, full):
    portions = [(1 << 20) // math.isqrt(rank ** lean) + 1 for rank in range(1, count + 1)]
    largest = reach if full else min(reach, max(-(-total // count), total * portions[0] // sum(portions)))
    least = 1 if total - largest >= count - 1 else 0
    holding, spare = [largest] + [least] * (count - 1), total - largest - least * (count - 1)
    while spare > 0:
        movable = [i for i in range(1, count) if holding[i] < largest] or [i for i in range(1, count) if holding[i] < reach]
        whole, left = sum([portions[i] for i in movable]), spare
        for i in movable:
            extra = min(reach - holding[i], max(1, left * portions[i] // whole), spare)
            holding[i] = holding[i] + extra
            spare = spare - extra
    return np.array(holding)


def scatter_about(own_key, dims, width, reach, split=(), kind=jnp.bfloat16):
    values = width * jax.random.normal(own_key, dims, jnp.float32)
    if split:
        values = values * levels(own_key, dims, split, -0.22, 0.18)
    return jnp.clip(values, -reach, reach).astype(kind)


def setup_inputs(seed: int = 0) -> dict:
    key_of = jax.random.split(jax.random.key(seed), 15)
    policy_hidden = scatter_about(key_of[0], (TOKENS, D), 1.0, 6.0, ((0, 8), (1, 4)))
    reference_hidden = scatter_about(key_of[1], (TOKENS, D), 1.0, 6.0, ((0, 8), (1, 4)))
    policy_norm_gain = jnp.clip(1.0 + 0.15 * jax.random.normal(key_of[2], (D,), jnp.float32), 0.25, 1.75)
    reference_norm_gain = jnp.clip(1.0 + 0.15 * jax.random.normal(key_of[3], (D,), jnp.float32), 0.25, 1.75)
    policy_router = draw_policy_router(jax.random.fold_in(key_of[14], 71), 0)
    reference_router = draw_reference_router(jax.random.fold_in(key_of[14], 71), 0)
    policy_gate = scatter_about(key_of[6], (EXPERTS, D, FF), D ** -0.5, 0.09375, ((0, 4), (1, 8)))
    policy_up = scatter_about(key_of[7], (EXPERTS, D, FF), D ** -0.5, 0.09375, ((0, 4), (1, 8)))
    policy_down = scatter_about(key_of[8], (EXPERTS, FF, D), FF ** -0.5, 0.0625, ((0, 4), (1, 8)))
    reference_gate = scatter_about(key_of[9], (EXPERTS, D, FF), D ** -0.5, 0.09375, ((0, 4), (1, 8)))
    reference_up = scatter_about(key_of[10], (EXPERTS, D, FF), D ** -0.5, 0.09375, ((0, 4), (1, 8)))
    reference_down = scatter_about(key_of[11], (EXPERTS, FF, D), FF ** -0.5, 0.0625, ((0, 4), (1, 8)))
    expert_ids_keys = jax.random.split(jax.random.fold_in(key_of[12], 1), TOKENS // TOK_DEV)
    expert_ids_turns = jax.random.permutation(jax.random.fold_in(key_of[12], 3), TOKENS // TOK_DEV)
    expert_ids = jax.vmap(lambda own, number: deal_out(jax.random.fold_in(key_of[12], 2), own, number, TOK_DEV, EXPERTS, TOP, CAP, 2))(expert_ids_keys, expert_ids_turns).reshape((TOKENS, TOP))
    lengths = draw_lengths(jax.random.fold_in(key_of[14], 71), 0)
    return {"policy_hidden": policy_hidden, "reference_hidden": reference_hidden, "policy_norm_gain": policy_norm_gain, "reference_norm_gain": reference_norm_gain, "policy_router": policy_router, "reference_router": reference_router, "policy_gate": policy_gate, "policy_up": policy_up, "policy_down": policy_down, "reference_gate": reference_gate, "reference_up": reference_up, "reference_down": reference_down, "expert_ids": expert_ids, "lengths": lengths}


EPSILON = 1e-05
KL_WEIGHT = 1.0
BALANCE_WEIGHT = 0.5

def normalize(hidden, norm_gain):
    values = hidden.astype(jnp.float32)
    meansq = lax.optimization_barrier(jnp.mean(values * values, axis=1, keepdims=True))
    return values * norm_gain * lax.rsqrt(meansq + EPSILON)

def expert_apply(operands):
    expert_rows, gate_weight, up_weight, down_weight = operands
    row_count = expert_rows.shape[0]
    gate_value = jnp.dot(expert_rows, gate_weight, preferred_element_type=jnp.float32)
    up_value = jnp.dot(expert_rows, up_weight, preferred_element_type=jnp.float32)
    hidden = (jax.nn.silu(gate_value) * up_value).astype(jnp.bfloat16)
    block_width = FF // N_DP
    hidden_blocks = hidden.reshape(row_count, N_DP, block_width).transpose(1, 0, 2)
    down_blocks = down_weight.reshape(N_DP, block_width, D)

    def add_block(running_total, operand_pair):
        block_part = jnp.dot(operand_pair[0], operand_pair[1], preferred_element_type=jnp.float32).astype(jnp.bfloat16)
        block_part = lax.optimization_barrier(block_part)
        return (running_total + block_part.astype(jnp.float32), None)
    running_total, _ = lax.scan(add_block, jnp.zeros((row_count, D), jnp.float32), (hidden_blocks, down_blocks))
    return running_total.astype(jnp.bfloat16)

def model_mixture(hidden, norm_gain, router, gate_weight, up_weight, down_weight, flat_slot, expert_ids, live_mask):
    normed = normalize(hidden, norm_gain)
    logits = jnp.dot(normed, router, precision=lax.Precision.HIGHEST)
    token_rows = normed.astype(jnp.bfloat16)
    route_rows = jnp.repeat(token_rows, TOP, axis=0)
    buffer = jnp.zeros((EXPERTS * N_DP * CAP, D), jnp.bfloat16).at[flat_slot].set(route_rows)
    buffer = buffer.reshape(EXPERTS, N_DP * CAP, D)
    outputs = lax.map(expert_apply, (buffer, gate_weight, up_weight, down_weight))
    picked = outputs.reshape(EXPERTS * N_DP * CAP, D)[flat_slot].reshape(TOKENS, TOP, D)
    matches = expert_ids[:, :, None] == jnp.arange(EXPERTS, dtype=jnp.int32)[None, None, :]
    chosen = lax.optimization_barrier(jnp.sum(jnp.where(matches, logits[:, None, :], 0.0), axis=2))
    gates = jax.nn.softmax(chosen, axis=1)
    mixed_rows = lax.optimization_barrier(jnp.sum(picked.astype(jnp.float32) * gates[:, :, None], axis=1)) * live_mask[:, None]
    return (mixed_rows.astype(jnp.bfloat16), logits)

def reference(policy_hidden, reference_hidden, policy_norm_gain, reference_norm_gain, policy_router, reference_router, policy_gate, policy_up, policy_down, reference_gate, reference_up, reference_down, expert_ids, lengths):
    position = jnp.arange(TOKENS, dtype=jnp.int32)
    live_mask = (position % SEG < jnp.repeat(lengths, SEG)).astype(jnp.float32)
    block_ids = expert_ids.reshape(N_DP, TOK_DEV * TOP)
    onehot = (block_ids[:, :, None] == jnp.arange(EXPERTS, dtype=jnp.int32)[None, None, :]).astype(jnp.int32)
    before = jnp.cumsum(onehot, axis=1) - onehot
    within = lax.optimization_barrier(jnp.sum(before * onehot, axis=2))
    block_index = jnp.arange(N_DP, dtype=jnp.int32)[:, None]
    flat_slot = (block_ids * (N_DP * CAP) + block_index * CAP + within).reshape(-1).astype(jnp.int32)
    policy_mixture, policy_logits = model_mixture(policy_hidden, policy_norm_gain, policy_router, policy_gate, policy_up, policy_down, flat_slot, expert_ids, live_mask)
    reference_mixture, reference_logits = model_mixture(reference_hidden, reference_norm_gain, reference_router, reference_gate, reference_up, reference_down, flat_slot, expert_ids, live_mask)
    policy_logprob = jax.nn.log_softmax(policy_logits, axis=1)
    reference_logprob = jax.nn.log_softmax(reference_logits, axis=1)
    policy_prob = jnp.exp(policy_logprob)
    token_kl = lax.optimization_barrier(jnp.sum(policy_prob * (policy_logprob - reference_logprob), axis=1)) * live_mask
    route_onehot = onehot.reshape(TOKENS, TOP, EXPERTS)
    counts = lax.optimization_barrier(jnp.sum(lax.optimization_barrier(jnp.sum(route_onehot, axis=1)).astype(jnp.float32) * live_mask[:, None], axis=0))
    probsum = lax.optimization_barrier(jnp.sum(policy_prob * live_mask[:, None], axis=0))
    kl_total = jnp.sum(token_kl)
    token_total = float(TOKENS)
    balance = EXPERTS * jnp.sum(counts / (TOP * token_total) * probsum / token_total)
    loss = KL_WEIGHT * kl_total / token_total + BALANCE_WEIGHT * balance
    return (policy_mixture, reference_mixture, token_kl, loss)
```

```python
import jax
import jax.numpy as jnp
from jax import lax
from jax.sharding import PartitionSpec as P

D = 4096
SEG = 32


EPSILON = 1e-05
KL_WEIGHT = 1.0
BALANCE_WEIGHT = 0.5


def router_terms(hidden, norm_gain, router):
    values = hidden.astype(jnp.float32)
    partial_logits = jnp.dot(values * norm_gain, router, precision=lax.Precision.HIGHEST)
    return (partial_logits, jnp.sum(values * values, axis=1))


def expert_terms(slice_rows, weights):
    results = []
    for model_index in range(len(weights)):
        gate_weight, up_weight, down_weight = weights[model_index]
        model_rows = slice_rows[:, model_index, :]
        values = []
        for weight in (gate_weight, up_weight):
            partial = jnp.dot(model_rows, weight, preferred_element_type=jnp.float32)
            values.append(
                lax.psum_scatter(
                    partial.astype(jnp.bfloat16), "dp", scatter_dimension=1, tiled=True
                ).astype(jnp.float32)
            )
        hidden = (jax.nn.silu(values[0]) * values[1]).astype(jnp.bfloat16)
        partial = jnp.dot(hidden, down_weight, preferred_element_type=jnp.float32)
        results.append(
            lax.psum_scatter(
                partial.astype(jnp.bfloat16), "dp", scatter_dimension=0, tiled=True
            )
        )
    return jnp.stack(results, axis=1)


def mixture(slot_rows, weights):
    expert_count, slot_count, models, feature_block = slot_rows.shape
    model_width = expert_count * feature_block
    arrived_rows = lax.all_to_all(slot_rows, "expert", split_axis=0, concat_axis=3, tiled=True)
    local_rows = arrived_rows.reshape(slot_count, models, model_width)
    slice_rows = lax.all_to_all(local_rows, "dp", split_axis=2, concat_axis=0, tiled=True)
    summed = expert_terms(slice_rows, weights)
    result = lax.all_to_all(
        summed.reshape(1, slot_count, models, model_width),
        "expert",
        split_axis=3,
        concat_axis=0,
        tiled=True,
    )
    return result


def per_device(
    policy_hidden,
    reference_hidden,
    policy_norm_gain,
    reference_norm_gain,
    policy_router,
    reference_router,
    policy_gate,
    policy_up,
    policy_down,
    reference_gate,
    reference_up,
    reference_down,
    expert_ids,
    lengths,
):
    expert_count = lax.axis_size("expert")
    token_count, feature_block = policy_hidden.shape
    route_count = expert_ids.shape[1]
    slot_count = 3 * token_count // expert_count
    token_total = float(token_count * lax.axis_size("dp"))
    policy_partial, policy_squares = router_terms(policy_hidden, policy_norm_gain, policy_router)
    reference_partial, reference_squares = router_terms(
        reference_hidden, reference_norm_gain, reference_router
    )
    policy_partial, reference_partial, policy_squares, reference_squares = lax.psum(
        (policy_partial, reference_partial, policy_squares, reference_squares), "expert"
    )
    policy_scale = lax.rsqrt(policy_squares / D + EPSILON)[:, None]
    reference_scale = lax.rsqrt(reference_squares / D + EPSILON)[:, None]
    policy_logits = policy_partial * policy_scale
    reference_logits = reference_partial * reference_scale
    policy_rows = (policy_hidden.astype(jnp.float32) * policy_norm_gain * policy_scale).astype(
        jnp.bfloat16
    )
    reference_rows = (
        reference_hidden.astype(jnp.float32) * reference_norm_gain * reference_scale
    ).astype(jnp.bfloat16)
    live_mask = (
        (jnp.arange(SEG, dtype=jnp.int32)[None, :] < lengths[:, None])
        .reshape(-1)
        .astype(jnp.float32)
    )
    flat_ids = expert_ids.reshape(-1)
    onehot = (flat_ids[:, None] == jnp.arange(expert_count, dtype=jnp.int32)[None, :]).astype(
        jnp.int32
    )
    before = jnp.cumsum(onehot, axis=0) - onehot
    target = flat_ids * slot_count + jnp.sum(before * onehot, axis=1)
    slot_index = jnp.arange(expert_count * slot_count, dtype=jnp.int32)
    select = jnp.any(
        slot_index[:, None, None] == target.reshape(token_count, route_count)[None, :, :], axis=2
    ).astype(jnp.bfloat16)

    def pair_gates(logits):
        matches = expert_ids[:, :, None] == jnp.arange(expert_count, dtype=jnp.int32)[None, None, :]
        chosen = jnp.sum(jnp.where(matches, logits[:, None, :], 0.0), axis=2)
        return jax.nn.softmax(chosen, axis=1)

    def combine(expert_output, gates):
        picked = jnp.take(
            expert_output.reshape(expert_count * slot_count, feature_block), target, axis=0
        )
        picked = picked.reshape(token_count, route_count, feature_block).astype(jnp.float32)
        mixed_rows = jnp.sum(picked * gates[:, :, None], axis=1) * live_mask[:, None]
        return mixed_rows.astype(jnp.bfloat16)

    stacked_rows = jnp.concatenate((policy_rows, reference_rows), axis=1)
    placed = jnp.dot(select, stacked_rows, preferred_element_type=jnp.float32).astype(jnp.bfloat16)
    expert_output = mixture(
        placed.reshape(expert_count, slot_count, 2, feature_block),
        (
            (policy_gate[0], policy_up[0], policy_down[0]),
            (reference_gate[0], reference_up[0], reference_down[0]),
        ),
    )
    policy_output = expert_output[:, :, 0, :]
    reference_output = expert_output[:, :, 1, :]
    policy_mixture = combine(policy_output, pair_gates(policy_logits))
    reference_mixture = combine(reference_output, pair_gates(reference_logits))
    policy_logprob = jax.nn.log_softmax(policy_logits, axis=1)
    reference_logprob = jax.nn.log_softmax(reference_logits, axis=1)
    policy_prob = jnp.exp(policy_logprob)
    token_kl = jnp.sum(policy_prob * (policy_logprob - reference_logprob), axis=1) * live_mask
    route_onehot = onehot.reshape(token_count, route_count, expert_count)
    counts = jnp.sum(jnp.sum(route_onehot, axis=1).astype(jnp.float32) * live_mask[:, None], axis=0)
    probsum = jnp.sum(policy_prob * live_mask[:, None], axis=0)
    counts, probsum, kl_total = lax.psum((counts, probsum, jnp.sum(token_kl)), "dp")
    balance = expert_count * jnp.sum(counts / (route_count * token_total) * probsum / token_total)
    loss = KL_WEIGHT * kl_total / token_total + BALANCE_WEIGHT * balance
    return (policy_mixture, reference_mixture, token_kl, loss)


def solution(mesh):
    in_specs = (
        P("dp", "expert"),
        P("dp", "expert"),
        P("expert"),
        P("expert"),
        P("expert", None),
        P("expert", None),
        P("expert", "dp", None),
        P("expert", "dp", None),
        P("expert", "dp", None),
        P("expert", "dp", None),
        P("expert", "dp", None),
        P("expert", "dp", None),
        P("dp", None),
        P("dp"),
    )
    out_specs = (P("dp", "expert"), P("dp", "expert"), P("dp"), P())
    return jax.shard_map(
        per_device, mesh=mesh, in_specs=in_specs, out_specs=out_specs, check_vma=False
    )
```
